32 devices in a mesh: gz: 8 (over z, y), xy: 4 (over x, core).
Axes of the slice: x: 2, y: 2, z: 4, core: 2. Of those that a mesh axis runs over, the one named last changes fastest.
Arguments:
- image: float32 [64, 512, 512], P('gz', 'xy'), may hold values from -6 to 6
- offsets: int32 [4, 64, 4, 4], P(None, 'gz', 'xy'), may hold values from -6 to 6
- frac_index: int32 [4, 64, 4, 4], P(None, 'gz', 'xy'), may hold values from 0 to 15
- fractions: float32 [16, 3], replicated, may hold values from 0 to 1
Outputs:
- transported: float32 [64, 512, 512], P('gz', 'xy')
The draws below stay inside these ranges and needn't reach their ends.
All inputs are finite; a program needn't handle non-finite values.
Results may differ from the reference program's by a relative error of at most 0.0003.
Values sent between devices are 32-bit elements; how exact they have to be, the bound alone decides.
A program may use at most 128 MiB of HBM per device.

```python
import jax
import jax.numpy as jnp
from jax import lax

BLOCK = 128
NBY = 4
STEPS = 4
FRACS = 16
NX = 512
NY = 512
NZ = 64


def place_ends(values, rng, least, top_value):
    spot = [jax.random.randint(jax.random.fold_in(rng, axis), (), 0, length) for axis, length in enumerate(values.shape)]
    widest = values.shape.index(max(values.shape))
    neighbour = spot[:widest] + [(spot[widest] + 1) % values.shape[widest]] + spot[widest + 1:]
    return values.at[tuple(spot)].set(least).at[tuple(neighbour)].set(top_value)


def block_levels(own_key, shape, cuts, low, largest):
    def one(axis_at, blocks):
        draws = jax.random.uniform(jax.random.fold_in(jax.random.fold_in(own_key, 6), axis_at), (blocks,), jnp.float32, low / len(cuts), largest / len(cuts))
        return jnp.repeat(jnp.exp(draws), shape[axis_at] // blocks).reshape((-1,) + (1,) * (len(shape) - axis_at - 1))

    loudness = one(*cuts[0])
    for cut in cuts[1:]:
        loudness = loudness * one(*cut)
    return loudness


def gaussian(stream_key, shape, width, limit, pieces=(), kind=jnp.bfloat16):
    values = jax.random.normal(stream_key, shape, jnp.float32) * width
    if len(pieces) > 0:
        values = block_levels(stream_key, shape, pieces, -0.22, 0.18) * values
    return jnp.clip(values, min=-limit, max=limit).astype(kind)


def setup_inputs(seed: int = 0) -> dict:
    key_list = jax.random.split(jax.random.key(seed), 5)
    return {
        "image": gaussian(key_list[0], (NZ, NX, NY), 1.0, 6.0, ((0, 8), (1, 4)), jnp.float32),
        "offsets": place_ends(jax.random.randint(key_list[1], (STEPS, NZ, NX // BLOCK, NBY), -6, 7), jax.random.fold_in(key_list[1], 1), -6, 6).astype(jnp.int32),
        "frac_index": place_ends(jax.random.randint(key_list[2], (STEPS, NZ, NX // BLOCK, NBY), 0, FRACS), jax.random.fold_in(key_list[2], 1), 0, FRACS - 1).astype(jnp.int32),
        "fractions": jnp.clip(jax.random.uniform(key_list[3], (FRACS, 3), jnp.float32, 0.0, 1.0), 0.0, 1.0),
    }


def cubic_weights(shares):
    return (-shares * (shares - 1.0) * (shares - 2.0) / 6.0,
            (shares + 1.0) * (shares - 1.0) * (shares - 2.0) / 2.0,
            -(shares + 1.0) * shares * (shares - 2.0) / 2.0,
            (shares + 1.0) * shares * (shares - 1.0) / 6.0)


def reference(image, offsets, frac_index, fractions):
    current = image
    block_rows = NX // BLOCK
    levels = jnp.arange(NZ, dtype=jnp.int32)
    for step_index in range(STEPS):
        padded = jnp.pad(current, ((0, 0), (2, 2), (2, 2)), mode="wrap")
        shifts_all = offsets[step_index]
        index_all = frac_index[step_index]

        def one_block(block_id):
            row_index = block_id // NBY
            col_index = block_id % NBY
            sub_volume = lax.dynamic_slice(padded, (jnp.int32(0), row_index * BLOCK, col_index * BLOCK), (NZ, BLOCK + 4, BLOCK + 4))
            shifts_now = shifts_all[:, row_index, col_index]
            picked = fractions[index_all[:, row_index, col_index]]
            zweights = cubic_weights(1.0 - picked[:, 0])
            xweights = cubic_weights(1.0 - picked[:, 1])
            yweights = cubic_weights(1.0 - picked[:, 2])
            merged = jnp.zeros((NZ, BLOCK + 4, BLOCK + 4), jnp.float32)
            for node in range(4):
                source = jnp.mod(levels - shifts_now - 2 + node, NZ).astype(jnp.int32)
                merged = merged + zweights[node][:, None, None] * sub_volume[source]
            along_y = jnp.zeros((NZ, BLOCK + 4, BLOCK), jnp.float32)
            for node in range(4):
                along_y = along_y + yweights[node][:, None, None] * merged[:, :, node:node + BLOCK]
            along_x = jnp.zeros((NZ, BLOCK, BLOCK), jnp.float32)
            for node in range(4):
                along_x = along_x + xweights[node][:, None, None] * along_y[:, node:node + BLOCK, :]
            return along_x

        blocks = lax.map(one_block, jnp.arange(block_rows * NBY, dtype=jnp.int32))
        current = blocks.reshape(block_rows, NBY, NZ, BLOCK, BLOCK).transpose(2, 0, 3, 1, 4).reshape(NZ, NX, NY)
    return current
```

```python
import functools

import jax
import jax.numpy as jnp
from jax import lax
from jax.experimental import pallas as pl
from jax.experimental.pallas import tpu as pltpu
from jax.sharding import PartitionSpec as P

MESH = pl.DeviceIdType.MESH
LANES = 128

HALO = 8


def along_path(place, n):
    if n % 2:
        return place
    layer, side = place // 2, place % 2
    return 2 * layer + side + (layer % 2) * (1 - 2 * side)


def slot_of(g, n, strip):
    g = along_path(g, n)
    return g + (strip % 2) * (n - 1 - 2 * g)


def device_at(slot, n, strip):
    return along_path(slot + (strip % 2) * (n - 1 - 2 * slot), n)


def fused_kernel(
    n, n_xy, steps,
    image_ref, meta_ref, fractions_ref, out_ref, meta_all_ref,
    landed, cells_a, cells_b, final, meta_s, shares, table,
    in_send, in_recv, meta_send, meta_recv, alt_sem, alt_recv, halo_send, halo_recv, cross_send,
    out_send, out_recv, local_sem,
):
    planes = image_ref.shape[0]
    width = image_ref.shape[1]
    nz = n * planes
    rows = final.shape[1]
    blocks = final.shape[2] // LANES
    pieces = 2 * n
    mid = n // 2
    me = lax.axis_index("gz")
    xy = lax.axis_index("xy")
    strip, half = xy // 2, lax.rem(xy, 2)
    piece = slot_of(me, n, strip) * 2 + half
    home = strip * 2 + piece // n
    part = lax.rem(piece, n)
    is_home = home == xy
    is_first = part == 0
    is_last = part == n - 1
    cross_up = piece == n - 1
    cross_down = piece == n
    near = (me // mid) * mid

    def holder(line):
        strip_at, piece_at = line // pieces, lax.rem(line, pieces)
        return device_at(piece_at // 2, n, strip_at), strip_at * 2 + lax.rem(piece_at, 2)

    line = strip * pieces + piece
    next_id = holder(lax.rem(line + 1, n * n_xy))
    prev_id = holder(lax.rem(line + n * n_xy - 1, n * n_xy))

    barrier = pltpu.get_barrier_semaphore()
    for i in range(1, pieces):
        other = lax.rem(half * n + me + i, pieces)
        pl.semaphore_signal(
            barrier, inc=1, device_id=(lax.rem(other, n), strip * 2 + other // n), device_id_type=MESH)
    for neighbour in (next_id, prev_id):
        pl.semaphore_signal(barrier, inc=1, device_id=neighbour, device_id_type=MESH)
    pl.semaphore_wait(barrier, pieces + 1)

    def share(i):
        return pl.ds(pl.multiple_of(i * rows, 8), rows)

    def slab(g):
        return pl.ds(g * planes, planes)

    def eight(g):
        return pl.ds(pl.multiple_of(g * 8, 8), 8)

    def taker(i):
        return holder(strip * pieces + half * n + i)

    own_rows = pl.ds(HALO, rows)
    low = -(-steps // 4) * 4
    high_rows, low_rows = pl.ds(0, HALO), pl.ds(HALO + rows, low)

    def meta_copy(i):
        return pltpu.make_async_remote_copy(
            src_ref=meta_ref, dst_ref=meta_all_ref.at[eight(me)],
            send_sem=meta_send.at[i], recv_sem=meta_recv.at[me], device_id=taker(i), device_id_type=MESH)

    def in_copy(i):
        return pltpu.make_async_remote_copy(
            src_ref=image_ref.at[:, share(i)], dst_ref=landed.at[slab(me), own_rows],
            send_sem=in_send.at[i], recv_sem=in_recv.at[me], device_id=taker(i), device_id_type=MESH)

    def meta_wait(g):
        return pltpu.make_async_copy(meta_ref, meta_all_ref.at[eight(g)], meta_recv.at[g])

    def in_wait(g):
        return pltpu.make_async_copy(image_ref.at[:, share(part)], landed.at[slab(g), own_rows], in_recv.at[g])

    def halo_copies(g):
        some = slab(g)
        return (
            (cross_up, pltpu.make_async_remote_copy(
                src_ref=landed.at[some, pl.ds(rows, HALO)], dst_ref=landed.at[some, high_rows],
                send_sem=halo_send.at[0, g], recv_sem=halo_recv.at[0, g],
                device_id=next_id, device_id_type=MESH)),
            (cross_down, pltpu.make_async_remote_copy(
                src_ref=landed.at[some, pl.ds(HALO, low)], dst_ref=landed.at[some, low_rows],
                send_sem=halo_send.at[1, g], recv_sem=halo_recv.at[1, g],
                device_id=prev_id, device_id_type=MESH)),
        )

    def halo_wait(g, side):
        lines = (high_rows, low_rows)[side]
        return pltpu.make_async_copy(
            image_ref.at[:, pl.ds(0, (HALO, low)[side])], landed.at[slab(g), lines], halo_recv.at[side, g])

    cross_id = holder(strip * pieces + n - half)
    cross_own = jnp.logical_and(cross_id[0] == me, cross_id[1] == xy)

    def cross_copies(side):
        lines = (high_rows, low_rows)[side]
        some = image_ref.at[:, pl.ds((width - HALO) * (1 - side), (HALO, low)[side])]
        there = landed.at[slab(me), lines]
        alt = meta_all_ref.at[eight(n + me)]
        return (
            (
                pltpu.make_async_remote_copy(
                    src_ref=meta_ref, dst_ref=alt, send_sem=cross_send.at[1], recv_sem=alt_recv.at[me],
                    device_id=cross_id, device_id_type=MESH),
                pltpu.make_async_remote_copy(
                    src_ref=some, dst_ref=there, send_sem=cross_send.at[0], recv_sem=halo_recv.at[side, me],
                    device_id=cross_id, device_id_type=MESH),
            ),
            (
                pltpu.make_async_copy(meta_ref, alt, alt_recv.at[me]),
                pltpu.make_async_copy(some, there, halo_recv.at[side, me]),
            ),
        )

    def out_copy(g):
        return pltpu.make_async_remote_copy(
            src_ref=final.at[slab(g)], dst_ref=out_ref.at[:, share(part)],
            send_sem=out_send.at[g], recv_sem=out_recv.at[part], device_id=(g, home), device_id_type=MESH)

    def out_wait(i):
        return pltpu.make_async_copy(final.at[slab(me)], out_ref.at[:, share(i)], out_recv.at[i])

    @pl.when(is_home)
    def _():
        meta_wait(me).start()
        in_wait(me).start()

    def send(make, i):
        @pl.when(jnp.logical_not(jnp.logical_and(is_home, i == part)))
        def _():
            make(i).start()

    @pl.loop(0, n)
    def _(turn):
        send(meta_copy, lax.rem(turn + me, n))

    def cross_each(remote, own):
        for side in range(2):
            @pl.when(half == side)
            def _():
                far, here = cross_copies(side)
                if own is not None:
                    @pl.when(cross_own)
                    def _():
                        for copy in here:
                            own(copy)

                @pl.when(jnp.logical_not(cross_own))
                def _():
                    for copy in far:
                        remote(copy)

    cross_each(lambda copy: copy.start(), lambda copy: copy.start())

    @pl.loop(0, mid)
    def _(turn):
        send(in_copy, (1 - half) * mid + lax.rem(turn + me, mid))

    @pl.loop(mid, n)
    def _(turn):
        send(in_copy, half * turn + (1 - half) * (n - 1 - turn))

    get_shares = pltpu.make_async_copy(fractions_ref, shares, local_sem.at[1])
    get_shares.start()
    get_shares.wait()
    for row in range(shares.shape[1]):
        rest = 1.0 - jnp.broadcast_to(shares[:, row : row + 1], (3, LANES))
        for node, weight_of in enumerate(cubic_weights(rest)):
            for axis in range(3):
                table[row, 4 * axis + node] = jnp.broadcast_to(weight_of[axis : axis + 1], (8, LANES))

    @pl.loop(0, n)
    def _(g):
        meta_wait(g).wait()

    own_meta, alt_meta = pl.ds(0, n * 8), pl.ds(n * 8, n * 8)
    outer_first = piece == 0
    outer_last = piece == pieces - 1

    def alt_copy(side):
        return pltpu.make_async_remote_copy(
            src_ref=meta_all_ref.at[own_meta], dst_ref=meta_all_ref.at[alt_meta],
            send_sem=alt_sem.at[0], recv_sem=alt_sem.at[1],
            device_id=(next_id, prev_id)[side], device_id_type=MESH)

    @pl.when(outer_last)
    def _():
        alt_copy(0).start()

    @pl.when(outer_first)
    def _():
        alt_copy(1).start()

    to_scalar = pltpu.make_async_copy(meta_all_ref.at[own_meta], meta_s.at[own_meta], local_sem.at[0])
    to_scalar.start()
    to_scalar.wait()

    @pl.loop(0, n)
    def _(turn):
        g = lax.rem(near + turn, n)
        in_wait(g).wait()
        for left_out, copy in halo_copies(g):
            @pl.when(jnp.logical_not(left_out))
            def _():
                copy.start()

    is_edge = jnp.logical_or(is_first, is_last)

    @pl.when(jnp.logical_or(outer_first, outer_last))
    def _():
        alt_copy(0).wait_recv()

    @pl.when(jnp.logical_or(cross_up, cross_down))
    def _():
        @pl.loop(0, n)
        def _(g):
            pltpu.make_async_copy(meta_ref, meta_all_ref.at[eight(n + g)], alt_recv.at[g]).wait()

    @pl.when(is_edge)
    def _():
        alt_to_scalar = pltpu.make_async_copy(meta_all_ref.at[alt_meta], meta_s.at[alt_meta], local_sem.at[0])
        alt_to_scalar.start()
        alt_to_scalar.wait()

    @pl.loop(0, n)
    def _(g):
        halo_wait(g, 0).wait()
        halo_wait(g, 1).wait()

    lane = lax.broadcasted_iota(jnp.int32, (8, LANES), 1)
    left = lane >= LANES // 2
    last_two = lane >= LANES - 2
    last_one = lane >= LANES - 1
    first = lane < 1

    def weights(base, s, group, inner, b):
        spot = (s * blocks + b) * planes + inner
        shift = meta_s[base + group * 8, spot]
        row = meta_s[base + group * 8 + 1, spot]
        return shift, [table[row, j] for j in range(12)]

    def read(s, at, b, start):
        if s == 0:
            return landed[at, pl.ds(start, 8), pl.ds(b * LANES, LANES)]
        source = cells_a if s % 2 == 1 else cells_b
        return source[at, b, pl.ds(start, 8), :]

    def stencil(s, k, b, shift, weight, start, stop, skip, count):
        spots = []
        for node in range(4):
            at = k - shift - 2 + node + 2 * nz
            spots.append(jnp.bitwise_and(at, nz - 1) if nz & (nz - 1) == 0 else lax.rem(at, nz))
        along = []
        for row in range(start, stop, 8):
            merged = None
            rim = None
            for node, at in enumerate(spots):
                own = weight[node] * read(s, at, b, row)
                side = weight[node] * jnp.where(
                    left, read(s, at, (b - 1) % blocks, row), read(s, at, (b + 1) % blocks, row))
                merged = own if merged is None else merged + own
                rim = side if rim is None else rim + side
            along.append(
                weight[8] * pltpu.roll(jnp.where(last_two, rim, merged), 2, 1)
                + weight[9] * pltpu.roll(jnp.where(last_one, rim, merged), 1, 1)
                + weight[10] * merged
                + weight[11] * pltpu.roll(jnp.where(first, rim, merged), LANES - 1, 1)
            )
        along = jnp.concatenate(along + along[-1:], axis=0)
        parts = []
        for row in range(0, count, 8):
            lines = min(8, along.shape[0] - (skip + row + 3))
            value = weight[4][:lines] * along[skip + row : skip + row + lines]
            for node in range(1, 4):
                value = value + weight[4 + node][:lines] * along[skip + row + node : skip + row + node + lines]
            parts.append(value[: min(lines, count - row)])
        return parts[0] if len(parts) == 1 else jnp.concatenate(parts, axis=0)

    def up(number):
        return -(-number // 8) * 8

    for s in range(steps):
        taken = rows + 3 * (steps - s)
        given = taken - 3
        target = cells_a if s % 2 == 0 else cells_b

        def plane(group, inner):
            k = group * planes + inner
            for b in range(blocks):
                shift, weight = weights(0, s, group, inner, b)
                value = stencil(s, k, b, shift, weight, 0, up(taken), 0, given)
                if s < steps - 1:
                    target[k, b, pl.ds(0, given), :] = value
                else:
                    final[k, :, pl.ds(b * LANES, LANES)] = value

        if s < steps - 1:
            @pl.loop(0, n)
            def _(group):
                @pl.loop(0, planes, unroll=4)
                def _(inner):
                    plane(group, inner)

            ahead = 2 * (steps - 1 - s)
            edge = rows + ahead
            for flag, start, stop, skip, row, count in (
                (is_first, 0, up(ahead + 3), 0, 0, ahead),
                (is_last, edge // 8 * 8, up(taken), edge % 8, edge, given - edge),
            ):
                @pl.when(flag)
                def _():
                    @pl.loop(0, n)
                    def _(group):
                        @pl.loop(0, planes, unroll=8)
                        def _(inner):
                            k = group * planes + inner
                            for b in range(blocks):
                                shift, weight = weights(n * 8, s, group, inner, b)
                                target[k, b, pl.ds(row, count), :] = stencil(
                                    s, k, b, shift, weight, start, stop, skip, count)
        else:
            for far in (1, 0):
                @pl.loop(0, mid)
                def _(turn):
                    to = lax.rem(near + far * mid, n) + lax.rem(turn + me, mid)

                    @pl.loop(0, planes, unroll=4)
                    def _(inner):
                        plane(to, inner)

                    @pl.when(jnp.logical_not(jnp.logical_and(is_home, to == me)))
                    def _():
                        out_copy(to).start()

    @pl.when(is_home)
    def _():
        out_wait(part).start()

    @pl.loop(0, n)
    def _(i):
        @pl.when(jnp.logical_not(jnp.logical_and(is_home, i == part)))
        def _():
            meta_copy(i).wait_send()
            in_copy(i).wait_send()

        for left_out, copy in halo_copies(i):
            @pl.when(jnp.logical_not(left_out))
            def _():
                copy.wait_send()

        @pl.when(jnp.logical_not(jnp.logical_and(is_home, i == me)))
        def _():
            out_copy(i).wait_send()

        out_wait(i).wait()

    cross_each(lambda copy: copy.wait_send(), None)

    @pl.when(jnp.logical_or(outer_first, outer_last))
    def _():
        alt_copy(0).wait_send()


def fused(image, offsets, frac_index, fractions, n, n_xy):
    planes, width, depth = image.shape
    steps, blocks = offsets.shape[0], offsets.shape[3]
    rows = width // n
    nz = n * planes
    length = steps * planes * blocks
    padded = -(-length // LANES) * LANES
    meta = jnp.transpose(jnp.stack([offsets, frac_index]), (0, 1, 3, 4, 2)).reshape(2, length)
    meta = jnp.pad(meta, ((0, 6), (0, padded - length)))
    table = fractions.T
    tall = -(-(rows + 3 * steps) // 8) * 8
    out, _ = pl.pallas_call(
        functools.partial(fused_kernel, n, n_xy, steps),
        out_shape=(
            jax.ShapeDtypeStruct(image.shape, jnp.float32),
            jax.ShapeDtypeStruct((2 * n * 8, padded), jnp.int32),
        ),
        in_specs=[
            pl.BlockSpec(memory_space=pl.ANY),
            pl.BlockSpec(memory_space=pl.ANY),
            pl.BlockSpec(memory_space=pl.ANY),
        ],
        out_specs=(pl.BlockSpec(memory_space=pl.ANY), pl.BlockSpec(memory_space=pl.ANY)),
        scratch_shapes=[
            pltpu.VMEM((nz, rows + 2 * HALO, depth), jnp.float32),
            pltpu.VMEM((nz, blocks, tall, LANES), jnp.float32),
            pltpu.VMEM((nz, blocks, tall, LANES), jnp.float32),
            pltpu.VMEM((nz, rows, depth), jnp.float32),
            pltpu.SMEM((2 * n * 8, padded), jnp.int32),
            pltpu.VMEM(table.shape, jnp.float32),
            pltpu.VMEM((table.shape[1], 12, 8, LANES), jnp.float32),
            pltpu.SemaphoreType.DMA((n,)),
            pltpu.SemaphoreType.DMA((n,)),
            pltpu.SemaphoreType.DMA((n,)),
            pltpu.SemaphoreType.DMA((n,)),
            pltpu.SemaphoreType.DMA((2,)),
            pltpu.SemaphoreType.DMA((n,)),
            pltpu.SemaphoreType.DMA((2, n)),
            pltpu.SemaphoreType.DMA((2, n)),
            pltpu.SemaphoreType.DMA((2,)),
            pltpu.SemaphoreType.DMA((n,)),
            pltpu.SemaphoreType.DMA((n,)),
            pltpu.SemaphoreType.DMA((2,)),
        ],
        compiler_params=pltpu.CompilerParams(
            collective_id=0, has_side_effects=True, vmem_limit_bytes=48 * 1024 * 1024),
    )(image, meta, table)
    return out


def extended(cells, sides, width):
    for axis, dim in sides:
        count = lax.axis_size(axis)
        head = lax.slice_in_dim(cells, 0, width, axis=dim)
        tail = lax.slice_in_dim(cells, cells.shape[dim] - width, cells.shape[dim], axis=dim)
        cells = jnp.concatenate(
            [
                lax.ppermute(tail, axis, [(i, (i + 1) % count) for i in range(count)]),
                cells,
                lax.ppermute(head, axis, [((i + 1) % count, i) for i in range(count)]),
            ],
            axis=dim,
        )
    return cells


def cubic_weights(shares):
    return (
        -shares * (shares - 1.0) * (shares - 2.0) / 6.0,
        (shares + 1.0) * (shares - 1.0) * (shares - 2.0) / 2.0,
        -(shares + 1.0) * shares * (shares - 2.0) / 2.0,
        (shares + 1.0) * shares * (shares - 1.0) / 6.0,
    )


def column_steps(image, offsets, frac_index, fractions):
    step_count = offsets.shape[0]
    all_shifts, all_index = (
        lax.all_gather(offsets, "gz", axis=1, tiled=True),
        lax.all_gather(frac_index, "gz", axis=1, tiled=True),
    )
    standing = jnp.swapaxes(
        lax.all_to_all(image, "gz", split_axis=2, concat_axis=0, tiled=True), 1, 2
    )
    total_planes = standing.shape[0]
    width_y = standing.shape[1]
    width_x = standing.shape[2]
    column_block = lax.axis_index("gz") * width_y // width_x
    block_pick = (jnp.arange(all_shifts.shape[3], dtype=jnp.int32) == column_block).astype(
        jnp.int32
    )
    levels = jnp.arange(total_planes, dtype=jnp.int32)
    table_rows = jnp.arange(fractions.shape[0], dtype=jnp.int32)
    for step_index in range(step_count):
        shifts_now = jnp.sum(all_shifts[step_index, :, 0, :] * block_pick[None, :], axis=1)
        index_now = jnp.sum(all_index[step_index, :, 0, :] * block_pick[None, :], axis=1)
        onehot = (index_now[:, None] == table_rows[None, :]).astype(jnp.float32)
        picked = jnp.dot(onehot, fractions, precision=lax.Precision.HIGHEST)
        zweights = cubic_weights(1.0 - picked[:, 0])
        xweights = cubic_weights(1.0 - picked[:, 1])
        yweights = cubic_weights(1.0 - picked[:, 2])
        rimmed = extended(standing, (("gz", 1), ("xy", 2)), 2)
        merged = jnp.zeros(rimmed.shape, jnp.float32)
        for node in range(4):
            source = jnp.mod(levels - shifts_now - 2 + node, total_planes)
            merged = merged + zweights[node][:, None, None] * jnp.take(rimmed, source, axis=0)
        along_y = jnp.zeros((total_planes, width_y, width_x + 4), jnp.float32)
        for node in range(4):
            along_y = along_y + yweights[node][:, None, None] * merged[:, node : node + width_y, :]
        along_x = jnp.zeros((total_planes, width_y, width_x), jnp.float32)
        for node in range(4):
            along_x = along_x + xweights[node][:, None, None] * along_y[:, :, node : node + width_x]
        standing = along_x
    return lax.all_to_all(
        jnp.swapaxes(standing, 1, 2), "gz", split_axis=0, concat_axis=2, tiled=True
    )


def solution(mesh):
    n, n_xy = mesh.shape["gz"], mesh.shape["xy"]

    def local(image, offsets, frac_index, fractions):
        planes, width, depth = image.shape
        block = depth // offsets.shape[3]
        if block == width == LANES and offsets.shape[2] == 1 and width % (8 * n) == 0 and n % 2 == 0 and n_xy % 2 == 0 and 2 * offsets.shape[0] <= HALO:
            return fused(image, offsets, frac_index, fractions, n, n_xy)
        return column_steps(image, offsets, frac_index, fractions)

    in_specs = (P("gz", "xy", None), P(None, "gz", "xy", None), P(None, "gz", "xy", None), P())
    out_specs = P("gz", "xy", None)
    return jax.shard_map(local, mesh=mesh, in_specs=in_specs, out_specs=out_specs, check_vma=False)
```

```python
import functools

import jax
import jax.numpy as jnp
from jax import lax
from jax.experimental import pallas as pl
from jax.experimental.pallas import tpu as pltpu
from jax.sharding import PartitionSpec as P

MESH = pl.DeviceIdType.MESH
LANES = 128

HALO = 8


def along_path(place, n):
    if n % 2:
        return place
    layer, side = place // 2, place % 2
    return 2 * layer + side + (layer % 2) * (1 - 2 * side)


def piece_of(g, core, n, pair):
    mid = n // 2
    slot = along_path(g, n)
    right = slot // mid
    place = slot + right * (n - 1 - 2 * slot)
    piece = core * (mid + place) + (1 - core) * (mid - 1 - place)
    flip = lax.rem(right + pair, 2)
    return piece + flip * (2 * n - 1 - 2 * piece)


def device_at(piece, n, pair):
    mid = n // 2
    piece = piece + lax.rem(pair, 2) * (2 * n - 1 - 2 * piece)
    right = piece // n
    piece = piece + right * (2 * n - 1 - 2 * piece)
    core = piece // mid
    place = core * (piece - mid) + (1 - core) * (mid - 1 - piece)
    return along_path(place + right * (n - 1 - 2 * place), n), pair * 2 + core


def fused_kernel(
    n, n_xy, steps,
    image_ref, meta_ref, fractions_ref, out_ref, meta_all_ref,
    landed, high, low, cells_a, cells_b, sides_a, sides_b, final, meta_s, shares, table,
    in_send, in_recv, meta_send, meta_recv, alt_sem, alt_recv, halo_send, halo_recv, cross_send,
    out_send, out_recv, local_sem,
):
    planes = image_ref.shape[0]
    width = image_ref.shape[1]
    nz = n * planes
    rows = final.shape[1]
    blocks = final.shape[2] // LANES
    pieces = 2 * n
    mid = n // 2
    me = lax.axis_index("gz")
    xy = lax.axis_index("xy")
    strip, half = xy // 2, lax.rem(xy, 2)
    piece = piece_of(me, half, n, strip)
    home = strip * 2 + piece // n
    part = lax.rem(piece, n)
    is_home = home == xy
    is_first = part == 0
    is_last = part == n - 1
    cross_up = piece == n - 1
    cross_down = piece == n
    near = (me // mid) * mid

    def holder(line):
        return device_at(lax.rem(line, pieces), n, line // pieces)

    line = strip * pieces + piece
    next_id = holder(lax.rem(line + 1, n * n_xy))
    prev_id = holder(lax.rem(line + n * n_xy - 1, n * n_xy))

    barrier = pltpu.get_barrier_semaphore()
    for i in range(1, pieces):
        other = lax.rem(half * n + me + i, pieces)
        pl.semaphore_signal(
            barrier, inc=1, device_id=(lax.rem(other, n), strip * 2 + other // n), device_id_type=MESH)
    for neighbour in (next_id, prev_id):
        pl.semaphore_signal(barrier, inc=1, device_id=neighbour, device_id_type=MESH)
    pl.semaphore_wait(barrier, pieces + 1)

    def share(i):
        return pl.ds(pl.multiple_of(i * rows, 8), rows)

    def slab(g):
        return pl.ds(g * planes, planes)

    def eight(g):
        return pl.ds(pl.multiple_of(g * 8, 8), 8)

    def taker(i):
        return holder(strip * pieces + half * n + i)

    beside = (high, low)
    deep = low.shape[1]

    def meta_copy(i):
        return pltpu.make_async_remote_copy(
            src_ref=meta_ref, dst_ref=meta_all_ref.at[eight(me)],
            send_sem=meta_send.at[i], recv_sem=meta_recv.at[me], device_id=taker(i), device_id_type=MESH)

    def in_copy(i):
        return pltpu.make_async_remote_copy(
            src_ref=image_ref.at[:, share(i)], dst_ref=landed.at[slab(me)],
            send_sem=in_send.at[i], recv_sem=in_recv.at[me], device_id=taker(i), device_id_type=MESH)

    def meta_wait(g):
        return pltpu.make_async_copy(meta_ref, meta_all_ref.at[eight(g)], meta_recv.at[g])

    def in_wait(g):
        return pltpu.make_async_copy(image_ref.at[:, share(part)], landed.at[slab(g)], in_recv.at[g])

    def halo_copies(g):
        some = slab(g)
        return (
            (cross_up, pltpu.make_async_remote_copy(
                src_ref=landed.at[some, pl.ds(rows - HALO, HALO)], dst_ref=high.at[some],
                send_sem=halo_send.at[0, g], recv_sem=halo_recv.at[0, g],
                device_id=next_id, device_id_type=MESH)),
            (cross_down, pltpu.make_async_remote_copy(
                src_ref=landed.at[some, pl.ds(0, deep)], dst_ref=low.at[some],
                send_sem=halo_send.at[1, g], recv_sem=halo_recv.at[1, g],
                device_id=prev_id, device_id_type=MESH)),
        )

    def halo_wait(g, side):
        return pltpu.make_async_copy(
            image_ref.at[:, pl.ds(0, (HALO, deep)[side])], beside[side].at[slab(g)], halo_recv.at[side, g])

    cross_id = holder(strip * pieces + n - half)
    cross_own = jnp.logical_and(cross_id[0] == me, cross_id[1] == xy)

    def cross_copies(side):
        some = image_ref.at[:, pl.ds((width - HALO) * (1 - side), (HALO, deep)[side])]
        there = beside[side].at[slab(me)]
        alt = meta_all_ref.at[eight(n + me)]
        return (
            (
                pltpu.make_async_remote_copy(
                    src_ref=meta_ref, dst_ref=alt, send_sem=cross_send.at[1], recv_sem=alt_recv.at[me],
                    device_id=cross_id, device_id_type=MESH),
                pltpu.make_async_remote_copy(
                    src_ref=some, dst_ref=there, send_sem=cross_send.at[0], recv_sem=halo_recv.at[side, me],
                    device_id=cross_id, device_id_type=MESH),
            ),
            (
                pltpu.make_async_copy(meta_ref, alt, alt_recv.at[me]),
                pltpu.make_async_copy(some, there, halo_recv.at[side, me]),
            ),
        )

    def out_copy(g):
        return pltpu.make_async_remote_copy(
            src_ref=final.at[slab(g)], dst_ref=out_ref.at[:, share(part)],
            send_sem=out_send.at[g], recv_sem=out_recv.at[part], device_id=(g, home), device_id_type=MESH)

    def out_wait(i):
        return pltpu.make_async_copy(final.at[slab(me)], out_ref.at[:, share(i)], out_recv.at[i])

    @pl.when(is_home)
    def _():
        meta_wait(me).start()
        in_wait(me).start()

    def send(make, i):
        @pl.when(jnp.logical_not(jnp.logical_and(is_home, i == part)))
        def _():
            make(i).start()

    @pl.loop(0, n)
    def _(turn):
        send(meta_copy, lax.rem(turn + me, n))

    def cross_each(remote, own):
        for side in range(2):
            @pl.when(half == side)
            def _():
                far, here = cross_copies(side)
                if own is not None:
                    @pl.when(cross_own)
                    def _():
                        for copy in here:
                            own(copy)

                @pl.when(jnp.logical_not(cross_own))
                def _():
                    for copy in far:
                        remote(copy)

    cross_each(lambda copy: copy.start(), lambda copy: copy.start())

    @pl.loop(0, mid)
    def _(turn):
        send(in_copy, (1 - half) * mid + lax.rem(turn + me, mid))

    in_middle = jnp.logical_and(piece >= mid, piece < pieces - mid)

    @pl.loop(mid, n)
    def _(turn):
        @pl.when(jnp.logical_not(in_middle))
        def _():
            send(in_copy, half * turn + (1 - half) * (n - 1 - turn))

    get_shares = pltpu.make_async_copy(fractions_ref, shares, local_sem.at[1])
    get_shares.start()
    get_shares.wait()
    for row in range(shares.shape[1]):
        rest = 1.0 - jnp.broadcast_to(shares[:, row : row + 1], (3, LANES))
        for node, weight_of in enumerate(cubic_weights(rest)):
            for axis in range(3):
                table[row, 4 * axis + node] = jnp.broadcast_to(weight_of[axis : axis + 1], (8, LANES))

    @pl.loop(0, n)
    def _(g):
        meta_wait(g).wait()

    own_meta, alt_meta = pl.ds(0, n * 8), pl.ds(n * 8, n * 8)
    outer_first = piece == 0
    outer_last = piece == pieces - 1

    def alt_copy(side):
        return pltpu.make_async_remote_copy(
            src_ref=meta_all_ref.at[own_meta], dst_ref=meta_all_ref.at[alt_meta],
            send_sem=alt_sem.at[0], recv_sem=alt_sem.at[1],
            device_id=(next_id, prev_id)[side], device_id_type=MESH)

    @pl.when(outer_last)
    def _():
        alt_copy(0).start()

    @pl.when(outer_first)
    def _():
        alt_copy(1).start()

    to_scalar = pltpu.make_async_copy(meta_all_ref.at[own_meta], meta_s.at[own_meta], local_sem.at[0])
    to_scalar.start()
    to_scalar.wait()

    @pl.loop(0, n)
    def _(turn):
        g = lax.rem(near + turn, n)
        in_wait(g).wait()
        for left_out, copy in halo_copies(g):
            @pl.when(jnp.logical_not(left_out))
            def _():
                copy.start()

        @pl.when(jnp.logical_and(in_middle, lax.rem(turn, 2) == 0))
        def _():
            later = mid + turn // 2
            send(in_copy, half * later + (1 - half) * (n - 1 - later))

    is_edge = jnp.logical_or(is_first, is_last)

    @pl.when(jnp.logical_or(outer_first, outer_last))
    def _():
        alt_copy(0).wait_recv()

    @pl.when(jnp.logical_or(cross_up, cross_down))
    def _():
        @pl.loop(0, n)
        def _(g):
            pltpu.make_async_copy(meta_ref, meta_all_ref.at[eight(n + g)], alt_recv.at[g]).wait()

    @pl.when(is_edge)
    def _():
        alt_to_scalar = pltpu.make_async_copy(meta_all_ref.at[alt_meta], meta_s.at[alt_meta], local_sem.at[0])
        alt_to_scalar.start()
        alt_to_scalar.wait()

    lane = lax.broadcasted_iota(jnp.int32, (8, LANES), 1)
    left = lane >= LANES // 2
    last_two = lane >= LANES - 2
    last_one = lane >= LANES - 1
    first = lane < 1

    def weights(base, s, group, inner, b):
        spot = (s * blocks + b) * planes + inner
        shift = meta_s[base + group * 8, spot]
        row = meta_s[base + group * 8 + 1, spot]
        return shift, [table[row, j] for j in range(12)]

    cells, sides = (cells_b, cells_a), (sides_b, sides_a)

    def read(s, at, b, row):
        if s > 0:
            return cells[s % 2][at, b, pl.ds(row, 8), :]
        lanes = pl.ds(b * LANES, LANES)
        if row < HALO:
            return high[at, :, lanes]
        if row < HALO + rows:
            return landed[at, pl.ds(row - HALO, 8), lanes]
        return low[at, :, lanes]

    def beyond(s, at, b, row):
        if s > 0:
            return sides[s % 2][at, b, pl.ds(row, 8), :]
        before = read(s, at, (b - 1) % blocks, row)
        return jnp.where(left[: before.shape[0]], before, read(s, at, (b + 1) % blocks, row))

    def across(s, k, b, shift, weight, start, stop):
        spots = []
        for node in range(4):
            at = k - shift - 2 + node + 2 * nz
            spots.append(jnp.bitwise_and(at, nz - 1) if nz & (nz - 1) == 0 else lax.rem(at, nz))
        along = []
        for row in range(start, stop, 8):
            lines = deep if s == 0 and row >= HALO + rows else 8
            own_weight = [w[:lines] for w in weight]
            merged = None
            rim = None
            for node, at in enumerate(spots):
                own = own_weight[node] * read(s, at, b, row)
                side = own_weight[node] * beyond(s, at, b, row)
                merged = own if merged is None else merged + own
                rim = side if rim is None else rim + side
            along.append(
                own_weight[8] * pltpu.roll(jnp.where(last_two[:lines], rim, merged), 2, 1)
                + own_weight[9] * pltpu.roll(jnp.where(last_one[:lines], rim, merged), 1, 1)
                + own_weight[10] * merged
                + own_weight[11] * pltpu.roll(jnp.where(first[:lines], rim, merged), LANES - 1, 1)
            )
        return along

    def down(weight, along, skip, count):
        if along[-1].shape[0] == 8:
            along = along + along[-1:]
        along = jnp.concatenate(along, axis=0)
        parts = []
        for row in range(0, count, 8):
            lines = min(8, along.shape[0] - (skip + row + 3))
            value = weight[4][:lines] * along[skip + row : skip + row + lines]
            for node in range(1, 4):
                value = value + weight[4 + node][:lines] * along[skip + row + node : skip + row + node + lines]
            parts.append(value[: min(lines, count - row)])
        return parts[0] if len(parts) == 1 else jnp.concatenate(parts, axis=0)

    def keep(s, k, row, values):
        count = values[0].shape[0]
        mine = lax.broadcasted_iota(jnp.int32, (count, LANES), 1) >= LANES // 2
        for b in range(blocks):
            there = pl.ds(row, count)
            cells[(s + 1) % 2][k, b, there, :] = values[b]
            sides[(s + 1) % 2][k, b, there, :] = jnp.where(
                mine, values[(b - 1) % blocks], values[(b + 1) % blocks])

    def each_plane(unroll, body):
        @pl.loop(0, n)
        def _(group):
            @pl.loop(0, planes, unroll=unroll)
            def _(inner):
                body(group, inner)

    def up(number):
        return -(-number // 8) * 8

    def inside(group, inner):
        k = group * planes + inner
        for b in range(blocks):
            shift, weight = weights(0, 0, group, inner, b)
            along = across(0, k, b, shift, weight, HALO, HALO + rows)
            for i, lines in enumerate(along):
                cells_b[k, b, pl.ds(HALO + 8 * i, 8), :] = lines

    each_plane(8, inside)

    @pl.loop(0, n)
    def _(g):
        halo_wait(g, 0).wait()
        halo_wait(g, 1).wait()

    for s in range(steps):
        taken = rows + 3 * (steps - s)
        given = taken - 3

        def values_of(group, inner):
            k = group * planes + inner
            values = []
            for b in range(blocks):
                shift, weight = weights(0, s, group, inner, b)
                if s == 0:
                    along = across(s, k, b, shift, weight, 0, HALO)
                    along += [cells_b[k, b, pl.ds(row, 8), :] for row in range(HALO, HALO + rows, 8)]
                    along += across(s, k, b, shift, weight, HALO + rows, up(taken))
                else:
                    along = across(s, k, b, shift, weight, 0, up(taken))
                values.append(down(weight, along, 0, given))
            return values

        if s < steps - 1:
            each_plane(8, lambda group, inner: keep(s, group * planes + inner, 0, values_of(group, inner)))

            ahead = 2 * (steps - 1 - s)
            edge = rows + ahead
            for flag, start, stop, skip, row, count in (
                (is_first, 0, up(ahead + 3), 0, 0, ahead),
                (is_last, edge // 8 * 8, up(taken), edge % 8, edge, given - edge),
            ):
                @pl.when(flag)
                def _():
                    def beside_plane(group, inner):
                        values = []
                        for b in range(blocks):
                            shift, weight = weights(n * 8, s, group, inner, b)
                            along = across(s, group * planes + inner, b, shift, weight, start, stop)
                            values.append(down(weight, along, skip, count))
                        keep(s, group * planes + inner, row, values)

                    each_plane(8, beside_plane)
        else:
            for far in (1, 0):
                @pl.loop(0, mid)
                def _(turn):
                    to = lax.rem(near + far * mid, n) + lax.rem(turn + me, mid)

                    @pl.loop(0, planes, unroll=8)
                    def _(inner):
                        for b, value in enumerate(values_of(to, inner)):
                            final[to * planes + inner, :, pl.ds(b * LANES, LANES)] = value

                    @pl.when(jnp.logical_not(jnp.logical_and(is_home, to == me)))
                    def _():
                        out_copy(to).start()

    @pl.when(is_home)
    def _():
        out_wait(part).start()

    @pl.loop(0, n)
    def _(i):
        @pl.when(jnp.logical_not(jnp.logical_and(is_home, i == part)))
        def _():
            meta_copy(i).wait_send()
            in_copy(i).wait_send()

        for left_out, copy in halo_copies(i):
            @pl.when(jnp.logical_not(left_out))
            def _():
                copy.wait_send()

        @pl.when(jnp.logical_not(jnp.logical_and(is_home, i == me)))
        def _():
            out_copy(i).wait_send()

        out_wait(i).wait()

    cross_each(lambda copy: copy.wait_send(), None)

    @pl.when(jnp.logical_or(outer_first, outer_last))
    def _():
        alt_copy(0).wait_send()


def fused(image, offsets, frac_index, fractions, n, n_xy):
    planes, width, depth = image.shape
    steps, blocks = offsets.shape[0], offsets.shape[3]
    rows = width // n
    nz = n * planes
    length = steps * planes * blocks
    padded = -(-length // LANES) * LANES
    meta = jnp.transpose(jnp.stack([offsets, frac_index]), (0, 1, 3, 4, 2)).reshape(2, length)
    meta = jnp.pad(meta, ((0, 6), (0, padded - length)))
    table = fractions.T
    tall = -(-(rows + 3 * steps) // 8) * 8
    out, _ = pl.pallas_call(
        functools.partial(fused_kernel, n, n_xy, steps),
        out_shape=(
            jax.ShapeDtypeStruct(image.shape, jnp.float32),
            jax.ShapeDtypeStruct((2 * n * 8, padded), jnp.int32),
        ),
        in_specs=[
            pl.BlockSpec(memory_space=pl.ANY),
            pl.BlockSpec(memory_space=pl.ANY),
            pl.BlockSpec(memory_space=pl.ANY),
        ],
        out_specs=(pl.BlockSpec(memory_space=pl.ANY), pl.BlockSpec(memory_space=pl.ANY)),
        scratch_shapes=[
            pltpu.VMEM((nz, rows, depth), jnp.float32),
            pltpu.VMEM((nz, HALO, depth), jnp.float32),
            pltpu.VMEM((nz, -(-steps // 4) * 4, depth), jnp.float32),
            pltpu.VMEM((nz, blocks, tall, LANES), jnp.float32),
            pltpu.VMEM((nz, blocks, tall, LANES), jnp.float32),
            pltpu.VMEM((nz, blocks, tall, LANES), jnp.float32),
            pltpu.VMEM((nz, blocks, tall, LANES), jnp.float32),
            pltpu.VMEM((nz, rows, depth), jnp.float32),
            pltpu.SMEM((2 * n * 8, padded), jnp.int32),
            pltpu.VMEM(table.shape, jnp.float32),
            pltpu.VMEM((table.shape[1], 12, 8, LANES), jnp.float32),
            pltpu.SemaphoreType.DMA((n,)),
            pltpu.SemaphoreType.DMA((n,)),
            pltpu.SemaphoreType.DMA((n,)),
            pltpu.SemaphoreType.DMA((n,)),
            pltpu.SemaphoreType.DMA((2,)),
            pltpu.SemaphoreType.DMA((n,)),
            pltpu.SemaphoreType.DMA((2, n)),
            pltpu.SemaphoreType.DMA((2, n)),
            pltpu.SemaphoreType.DMA((2,)),
            pltpu.SemaphoreType.DMA((n,)),
            pltpu.SemaphoreType.DMA((n,)),
            pltpu.SemaphoreType.DMA((2,)),
        ],
        compiler_params=pltpu.CompilerParams(
            collective_id=0, has_side_effects=True, vmem_limit_bytes=48 * 1024 * 1024),
    )(image, meta, table)
    return out


def extended(cells, sides, width):
    for axis, dim in sides:
        count = lax.axis_size(axis)
        head = lax.slice_in_dim(cells, 0, width, axis=dim)
        tail = lax.slice_in_dim(cells, cells.shape[dim] - width, cells.shape[dim], axis=dim)
        cells = jnp.concatenate(
            [
                lax.ppermute(tail, axis, [(i, (i + 1) % count) for i in range(count)]),
                cells,
                lax.ppermute(head, axis, [((i + 1) % count, i) for i in range(count)]),
            ],
            axis=dim,
        )
    return cells


def cubic_weights(shares):
    return (
        -shares * (shares - 1.0) * (shares - 2.0) / 6.0,
        (shares + 1.0) * (shares - 1.0) * (shares - 2.0) / 2.0,
        -(shares + 1.0) * shares * (shares - 2.0) / 2.0,
        (shares + 1.0) * shares * (shares - 1.0) / 6.0,
    )


def column_steps(image, offsets, frac_index, fractions):
    step_count = offsets.shape[0]
    all_shifts, all_index = (
        lax.all_gather(offsets, "gz", axis=1, tiled=True),
        lax.all_gather(frac_index, "gz", axis=1, tiled=True),
    )
    standing = jnp.swapaxes(
        lax.all_to_all(image, "gz", split_axis=2, concat_axis=0, tiled=True), 1, 2
    )
    total_planes = standing.shape[0]
    width_y = standing.shape[1]
    width_x = standing.shape[2]
    column_block = lax.axis_index("gz") * width_y // width_x
    block_pick = (jnp.arange(all_shifts.shape[3], dtype=jnp.int32) == column_block).astype(
        jnp.int32
    )
    levels = jnp.arange(total_planes, dtype=jnp.int32)
    table_rows = jnp.arange(fractions.shape[0], dtype=jnp.int32)
    for step_index in range(step_count):
        shifts_now = jnp.sum(all_shifts[step_index, :, 0, :] * block_pick[None, :], axis=1)
        index_now = jnp.sum(all_index[step_index, :, 0, :] * block_pick[None, :], axis=1)
        onehot = (index_now[:, None] == table_rows[None, :]).astype(jnp.float32)
        picked = jnp.dot(onehot, fractions, precision=lax.Precision.HIGHEST)
        zweights = cubic_weights(1.0 - picked[:, 0])
        xweights = cubic_weights(1.0 - picked[:, 1])
        yweights = cubic_weights(1.0 - picked[:, 2])
        rimmed = extended(standing, (("gz", 1), ("xy", 2)), 2)
        merged = jnp.zeros(rimmed.shape, jnp.float32)
        for node in range(4):
            source = jnp.mod(levels - shifts_now - 2 + node, total_planes)
            merged = merged + zweights[node][:, None, None] * jnp.take(rimmed, source, axis=0)
        along_y = jnp.zeros((total_planes, width_y, width_x + 4), jnp.float32)
        for node in range(4):
            along_y = along_y + yweights[node][:, None, None] * merged[:, node : node + width_y, :]
        along_x = jnp.zeros((total_planes, width_y, width_x), jnp.float32)
        for node in range(4):
            along_x = along_x + xweights[node][:, None, None] * along_y[:, :, node : node + width_x]
        standing = along_x
    return lax.all_to_all(
        jnp.swapaxes(standing, 1, 2), "gz", split_axis=0, concat_axis=2, tiled=True
    )


def solution(mesh):
    n, n_xy = mesh.shape["gz"], mesh.shape["xy"]

    def local(image, offsets, frac_index, fractions):
        planes, width, depth = image.shape
        block = depth // offsets.shape[3]
        if block == width == LANES and offsets.shape[2] == 1 and width % (8 * n) == 0 and n % 2 == 0 and n_xy % 2 == 0 and 2 * offsets.shape[0] <= HALO:
            return fused(image, offsets, frac_index, fractions, n, n_xy)
        return column_steps(image, offsets, frac_index, fractions)

    in_specs = (P("gz", "xy", None), P(None, "gz", "xy", None), P(None, "gz", "xy", None), P())
    out_specs = P("gz", "xy", None)
    return jax.shard_map(local, mesh=mesh, in_specs=in_specs, out_specs=out_specs, check_vma=False)
```

```python
import functools

import jax
import jax.numpy as jnp
from jax import lax
from jax.experimental import pallas as pl
from jax.experimental.pallas import tpu as pltpu
from jax.sharding import PartitionSpec as P

MESH = pl.DeviceIdType.MESH
LANES = 128

HALO = 8


def along_path(place, n):
    if n % 2:
        return place
    layer, side = place // 2, place % 2
    return 2 * layer + side + (layer % 2) * (1 - 2 * side)


def piece_of(g, core, n, pair):
    mid = n // 2
    slot = along_path(g, n)
    right = slot // mid
    place = slot + right * (n - 1 - 2 * slot)
    piece = core * (mid + place) + (1 - core) * (mid - 1 - place)
    flip = lax.rem(right + pair, 2)
    return piece + flip * (2 * n - 1 - 2 * piece)


def device_at(piece, n, pair):
    mid = n // 2
    piece = piece + lax.rem(pair, 2) * (2 * n - 1 - 2 * piece)
    right = piece // n
    piece = piece + right * (2 * n - 1 - 2 * piece)
    core = piece // mid
    place = core * (piece - mid) + (1 - core) * (mid - 1 - piece)
    return along_path(place + right * (n - 1 - 2 * place), n), pair * 2 + core


def fused_kernel(
    n, n_xy, steps,
    image_ref, meta_ref, fractions_ref, out_ref, meta_all_ref,
    landed, high, low, cells_a, cells_b, sides_a, sides_b, final, meta_s, shares, table,
    in_send, in_recv, meta_send, meta_recv, alt_sem, alt_recv, halo_send, halo_recv, cross_send,
    out_send, out_recv, local_sem,
):
    planes = image_ref.shape[0]
    width = image_ref.shape[1]
    nz = n * planes
    rows = final.shape[1]
    blocks = final.shape[2] // LANES
    pieces = 2 * n
    mid = n // 2
    me = lax.axis_index("gz")
    xy = lax.axis_index("xy")
    strip, half = xy // 2, lax.rem(xy, 2)
    piece = piece_of(me, half, n, strip)
    home = strip * 2 + piece // n
    part = lax.rem(piece, n)
    is_home = home == xy
    is_first = part == 0
    is_last = part == n - 1
    cross_up = piece == n - 1
    cross_down = piece == n
    near = (me // mid) * mid

    def holder(line):
        return device_at(lax.rem(line, pieces), n, line // pieces)

    line = strip * pieces + piece
    next_id = holder(lax.rem(line + 1, n * n_xy))
    prev_id = holder(lax.rem(line + n * n_xy - 1, n * n_xy))

    barrier = pltpu.get_barrier_semaphore()
    for i in range(1, pieces):
        other = lax.rem(half * n + me + i, pieces)
        pl.semaphore_signal(
            barrier, inc=1, device_id=(lax.rem(other, n), strip * 2 + other // n), device_id_type=MESH)
    for neighbour in (next_id, prev_id):
        pl.semaphore_signal(barrier, inc=1, device_id=neighbour, device_id_type=MESH)
    pl.semaphore_wait(barrier, pieces + 1)

    def share(i):
        return pl.ds(pl.multiple_of(i * rows, 8), rows)

    def slab(g):
        return pl.ds(g * planes, planes)

    def eight(g):
        return pl.ds(pl.multiple_of(g * 8, 8), 8)

    def taker(i):
        return holder(strip * pieces + half * n + i)

    beside = (high, low)
    deep = low.shape[1]

    def meta_copy(i):
        return pltpu.make_async_remote_copy(
            src_ref=meta_ref, dst_ref=meta_all_ref.at[eight(me)],
            send_sem=meta_send.at[i], recv_sem=meta_recv.at[me], device_id=taker(i), device_id_type=MESH)

    def in_copy(i):
        return pltpu.make_async_remote_copy(
            src_ref=image_ref.at[:, share(i)], dst_ref=landed.at[slab(me)],
            send_sem=in_send.at[i], recv_sem=in_recv.at[me], device_id=taker(i), device_id_type=MESH)

    def meta_wait(g):
        return pltpu.make_async_copy(meta_ref, meta_all_ref.at[eight(g)], meta_recv.at[g])

    def in_wait(g):
        return pltpu.make_async_copy(image_ref.at[:, share(part)], landed.at[slab(g)], in_recv.at[g])

    def halo_copies(g):
        some = slab(g)
        return (
            (cross_up, pltpu.make_async_remote_copy(
                src_ref=landed.at[some, pl.ds(rows - HALO, HALO)], dst_ref=high.at[some],
                send_sem=halo_send.at[0, g], recv_sem=halo_recv.at[0, g],
                device_id=next_id, device_id_type=MESH)),
            (cross_down, pltpu.make_async_remote_copy(
                src_ref=landed.at[some, pl.ds(0, deep)], dst_ref=low.at[some],
                send_sem=halo_send.at[1, g], recv_sem=halo_recv.at[1, g],
                device_id=prev_id, device_id_type=MESH)),
        )

    def halo_wait(g, side):
        return pltpu.make_async_copy(
            image_ref.at[:, pl.ds(0, (HALO, deep)[side])], beside[side].at[slab(g)], halo_recv.at[side, g])

    cross_id = holder(strip * pieces + n - half)
    cross_own = jnp.logical_and(cross_id[0] == me, cross_id[1] == xy)

    def cross_copies(side):
        some = image_ref.at[:, pl.ds((width - HALO) * (1 - side), (HALO, deep)[side])]
        there = beside[side].at[slab(me)]
        alt = meta_all_ref.at[eight(n + me)]
        return (
            (
                pltpu.make_async_remote_copy(
                    src_ref=meta_ref, dst_ref=alt, send_sem=cross_send.at[1], recv_sem=alt_recv.at[me],
                    device_id=cross_id, device_id_type=MESH),
                pltpu.make_async_remote_copy(
                    src_ref=some, dst_ref=there, send_sem=cross_send.at[0], recv_sem=halo_recv.at[side, me],
                    device_id=cross_id, device_id_type=MESH),
            ),
            (
                pltpu.make_async_copy(meta_ref, alt, alt_recv.at[me]),
                pltpu.make_async_copy(some, there, halo_recv.at[side, me]),
            ),
        )

    def out_copy(g):
        return pltpu.make_async_remote_copy(
            src_ref=final.at[slab(g)], dst_ref=out_ref.at[:, share(part)],
            send_sem=out_send.at[g], recv_sem=out_recv.at[part], device_id=(g, home), device_id_type=MESH)

    def out_wait(i):
        return pltpu.make_async_copy(final.at[slab(me)], out_ref.at[:, share(i)], out_recv.at[i])

    @pl.when(is_home)
    def _():
        meta_wait(me).start()
        in_wait(me).start()

    def send(make, i):
        @pl.when(jnp.logical_not(jnp.logical_and(is_home, i == part)))
        def _():
            make(i).start()

    @pl.loop(0, n)
    def _(turn):
        send(meta_copy, lax.rem(turn + me, n))

    def cross_each(remote, own):
        for side in range(2):
            @pl.when(half == side)
            def _():
                far, here = cross_copies(side)
                if own is not None:
                    @pl.when(cross_own)
                    def _():
                        for copy in here:
                            own(copy)

                @pl.when(jnp.logical_not(cross_own))
                def _():
                    for copy in far:
                        remote(copy)

    @pl.loop(0, mid)
    def _(turn):
        send(in_copy, (1 - half) * mid + lax.rem(turn + me, mid))

    cross_each(lambda copy: copy.start(), lambda copy: copy.start())

    in_middle = jnp.logical_and(piece >= mid, piece < pieces - mid)

    @pl.loop(mid, n)
    def _(turn):
        @pl.when(jnp.logical_not(in_middle))
        def _():
            send(in_copy, half * turn + (1 - half) * (n - 1 - turn))

    get_shares = pltpu.make_async_copy(fractions_ref, shares, local_sem.at[1])
    get_shares.start()
    get_shares.wait()
    for row in range(shares.shape[1]):
        rest = 1.0 - jnp.broadcast_to(shares[:, row : row + 1], (3, LANES))
        for node, weight_of in enumerate(cubic_weights(rest)):
            for axis in range(3):
                table[row, 4 * axis + node] = jnp.broadcast_to(weight_of[axis : axis + 1], (8, LANES))

    @pl.loop(0, n)
    def _(g):
        meta_wait(g).wait()

    own_meta, alt_meta = pl.ds(0, n * 8), pl.ds(n * 8, n * 8)
    outer_first = piece == 0
    outer_last = piece == pieces - 1

    def alt_copy(side):
        return pltpu.make_async_remote_copy(
            src_ref=meta_all_ref.at[own_meta], dst_ref=meta_all_ref.at[alt_meta],
            send_sem=alt_sem.at[0], recv_sem=alt_sem.at[1],
            device_id=(next_id, prev_id)[side], device_id_type=MESH)

    @pl.when(outer_last)
    def _():
        alt_copy(0).start()

    @pl.when(outer_first)
    def _():
        alt_copy(1).start()

    to_scalar = pltpu.make_async_copy(meta_all_ref.at[own_meta], meta_s.at[own_meta], local_sem.at[0])
    to_scalar.start()
    to_scalar.wait()

    @pl.loop(0, n)
    def _(turn):
        g = lax.rem(near + turn, n)
        in_wait(g).wait()
        for left_out, copy in halo_copies(g):
            @pl.when(jnp.logical_not(left_out))
            def _():
                copy.start()

        @pl.when(jnp.logical_and(in_middle, lax.rem(turn, 2) == 0))
        def _():
            later = mid + turn // 2
            send(in_copy, half * later + (1 - half) * (n - 1 - later))

    is_edge = jnp.logical_or(is_first, is_last)

    @pl.when(jnp.logical_or(outer_first, outer_last))
    def _():
        alt_copy(0).wait_recv()

    @pl.when(jnp.logical_or(cross_up, cross_down))
    def _():
        @pl.loop(0, n)
        def _(g):
            pltpu.make_async_copy(meta_ref, meta_all_ref.at[eight(n + g)], alt_recv.at[g]).wait()

    @pl.when(is_edge)
    def _():
        alt_to_scalar = pltpu.make_async_copy(meta_all_ref.at[alt_meta], meta_s.at[alt_meta], local_sem.at[0])
        alt_to_scalar.start()
        alt_to_scalar.wait()

    lane = lax.broadcasted_iota(jnp.int32, (8, LANES), 1)
    left = lane >= LANES // 2
    last_two = lane >= LANES - 2
    last_one = lane >= LANES - 1
    first = lane < 1

    def weights(base, s, group, inner, b):
        spot = (s * blocks + b) * planes + inner
        shift = meta_s[base + group * 8, spot]
        row = meta_s[base + group * 8 + 1, spot]
        return shift, [table[row, j] for j in range(12)]

    cells, sides = (cells_b, cells_a), (sides_b, sides_a)

    def read(s, at, b, row):
        if s > 0:
            return cells[s % 2][at, b, pl.ds(row, 8), :]
        lanes = pl.ds(b * LANES, LANES)
        if row < HALO:
            return high[at, :, lanes]
        if row < HALO + rows:
            return landed[at, pl.ds(row - HALO, 8), lanes]
        return low[at, :, lanes]

    def beyond(s, at, b, row):
        if s > 0:
            return sides[s % 2][at, b, pl.ds(row, 8), :]
        before = read(s, at, (b - 1) % blocks, row)
        return jnp.where(left[: before.shape[0]], before, read(s, at, (b + 1) % blocks, row))

    def across(s, k, b, shift, weight, start, stop):
        spots = []
        for node in range(4):
            at = k - shift - 2 + node + 2 * nz
            spots.append(jnp.bitwise_and(at, nz - 1) if nz & (nz - 1) == 0 else lax.rem(at, nz))
        along = []
        for row in range(start, stop, 8):
            lines = deep if s == 0 and row >= HALO + rows else 8
            own_weight = [w[:lines] for w in weight]
            merged = None
            rim = None
            for node, at in enumerate(spots):
                own = own_weight[node] * read(s, at, b, row)
                side = own_weight[node] * beyond(s, at, b, row)
                merged = own if merged is None else merged + own
                rim = side if rim is None else rim + side
            along.append(
                own_weight[8] * pltpu.roll(jnp.where(last_two[:lines], rim, merged), 2, 1)
                + own_weight[9] * pltpu.roll(jnp.where(last_one[:lines], rim, merged), 1, 1)
                + own_weight[10] * merged
                + own_weight[11] * pltpu.roll(jnp.where(first[:lines], rim, merged), LANES - 1, 1)
            )
        return along

    def down(weight, along, skip, count):
        if along[-1].shape[0] == 8:
            along = along + along[-1:]
        along = jnp.concatenate(along, axis=0)
        parts = []
        for row in range(0, count, 8):
            lines = min(8, along.shape[0] - (skip + row + 3))
            value = weight[4][:lines] * along[skip + row : skip + row + lines]
            for node in range(1, 4):
                value = value + weight[4 + node][:lines] * along[skip + row + node : skip + row + node + lines]
            parts.append(value[: min(lines, count - row)])
        return parts[0] if len(parts) == 1 else jnp.concatenate(parts, axis=0)

    def keep(s, k, row, values):
        count = values[0].shape[0]
        mine = lax.broadcasted_iota(jnp.int32, (count, LANES), 1) >= LANES // 2
        for b in range(blocks):
            there = pl.ds(row, count)
            cells[(s + 1) % 2][k, b, there, :] = values[b]
            sides[(s + 1) % 2][k, b, there, :] = jnp.where(
                mine, values[(b - 1) % blocks], values[(b + 1) % blocks])

    def each_plane(unroll, body):
        @pl.loop(0, n)
        def _(group):
            @pl.loop(0, planes, unroll=unroll)
            def _(inner):
                body(group, inner)

    def up(number):
        return -(-number // 8) * 8

    def inside(group, inner):
        k = group * planes + inner
        for b in range(blocks):
            shift, weight = weights(0, 0, group, inner, b)
            along = across(0, k, b, shift, weight, HALO, HALO + rows)
            for i, lines in enumerate(along):
                cells_b[k, b, pl.ds(HALO + 8 * i, 8), :] = lines

    each_plane(8, inside)

    @pl.loop(0, n)
    def _(g):
        halo_wait(g, 0).wait()
        halo_wait(g, 1).wait()

    for s in range(steps):
        taken = rows + 3 * (steps - s)
        given = taken - 3

        def values_of(group, inner):
            k = group * planes + inner
            values = []
            for b in range(blocks):
                shift, weight = weights(0, s, group, inner, b)
                if s == 0:
                    along = across(s, k, b, shift, weight, 0, HALO)
                    along += [cells_b[k, b, pl.ds(row, 8), :] for row in range(HALO, HALO + rows, 8)]
                    along += across(s, k, b, shift, weight, HALO + rows, up(taken))
                else:
                    along = across(s, k, b, shift, weight, 0, up(taken))
                values.append(down(weight, along, 0, given))
            return values

        if s < steps - 1:
            each_plane(8, lambda group, inner: keep(s, group * planes + inner, 0, values_of(group, inner)))

            ahead = 2 * (steps - 1 - s)
            edge = rows + ahead
            for flag, start, stop, skip, row, count in (
                (is_first, 0, up(ahead + 3), 0, 0, ahead),
                (is_last, edge // 8 * 8, up(taken), edge % 8, edge, given - edge),
            ):
                @pl.when(flag)
                def _():
                    def beside_plane(group, inner):
                        values = []
                        for b in range(blocks):
                            shift, weight = weights(n * 8, s, group, inner, b)
                            along = across(s, group * planes + inner, b, shift, weight, start, stop)
                            values.append(down(weight, along, skip, count))
                        keep(s, group * planes + inner, row, values)

                    each_plane(8, beside_plane)
        else:
            for far in (1, 0):
                @pl.loop(0, mid)
                def _(turn):
                    to = lax.rem(near + far * mid, n) + lax.rem(turn + me + 2 * half, mid)

                    @pl.loop(0, planes, unroll=8)
                    def _(inner):
                        for b, value in enumerate(values_of(to, inner)):
                            final[to * planes + inner, :, pl.ds(b * LANES, LANES)] = value

                    @pl.when(jnp.logical_not(jnp.logical_and(is_home, to == me)))
                    def _():
                        out_copy(to).start()

    @pl.when(is_home)
    def _():
        out_wait(part).start()

    @pl.loop(0, n)
    def _(i):
        @pl.when(jnp.logical_not(jnp.logical_and(is_home, i == part)))
        def _():
            meta_copy(i).wait_send()
            in_copy(i).wait_send()

        for left_out, copy in halo_copies(i):
            @pl.when(jnp.logical_not(left_out))
            def _():
                copy.wait_send()

        @pl.when(jnp.logical_not(jnp.logical_and(is_home, i == me)))
        def _():
            out_copy(i).wait_send()

        out_wait(i).wait()

    cross_each(lambda copy: copy.wait_send(), None)

    @pl.when(jnp.logical_or(outer_first, outer_last))
    def _():
        alt_copy(0).wait_send()


def fused(image, offsets, frac_index, fractions, n, n_xy):
    planes, width, depth = image.shape
    steps, blocks = offsets.shape[0], offsets.shape[3]
    rows = width // n
    nz = n * planes
    length = steps * planes * blocks
    padded = -(-length // LANES) * LANES
    meta = jnp.transpose(jnp.stack([offsets, frac_index]), (0, 1, 3, 4, 2)).reshape(2, length)
    meta = jnp.pad(meta, ((0, 6), (0, padded - length)))
    table = fractions.T
    tall = -(-(rows + 3 * steps) // 8) * 8
    out, _ = pl.pallas_call(
        functools.partial(fused_kernel, n, n_xy, steps),
        out_shape=(
            jax.ShapeDtypeStruct(image.shape, jnp.float32),
            jax.ShapeDtypeStruct((2 * n * 8, padded), jnp.int32),
        ),
        in_specs=[
            pl.BlockSpec(memory_space=pl.ANY),
            pl.BlockSpec(memory_space=pl.ANY),
            pl.BlockSpec(memory_space=pl.ANY),
        ],
        out_specs=(pl.BlockSpec(memory_space=pl.ANY), pl.BlockSpec(memory_space=pl.ANY)),
        scratch_shapes=[
            pltpu.VMEM((nz, rows, depth), jnp.float32),
            pltpu.VMEM((nz, HALO, depth), jnp.float32),
            pltpu.VMEM((nz, -(-steps // 4) * 4, depth), jnp.float32),
            pltpu.VMEM((nz, blocks, tall, LANES), jnp.float32),
            pltpu.VMEM((nz, blocks, tall, LANES), jnp.float32),
            pltpu.VMEM((nz, blocks, tall, LANES), jnp.float32),
            pltpu.VMEM((nz, blocks, tall, LANES), jnp.float32),
            pltpu.VMEM((nz, rows, depth), jnp.float32),
            pltpu.SMEM((2 * n * 8, padded), jnp.int32),
            pltpu.VMEM(table.shape, jnp.float32),
            pltpu.VMEM((table.shape[1], 12, 8, LANES), jnp.float32),
            pltpu.SemaphoreType.DMA((n,)),
            pltpu.SemaphoreType.DMA((n,)),
            pltpu.SemaphoreType.DMA((n,)),
            pltpu.SemaphoreType.DMA((n,)),
            pltpu.SemaphoreType.DMA((2,)),
            pltpu.SemaphoreType.DMA((n,)),
            pltpu.SemaphoreType.DMA((2, n)),
            pltpu.SemaphoreType.DMA((2, n)),
            pltpu.SemaphoreType.DMA((2,)),
            pltpu.SemaphoreType.DMA((n,)),
            pltpu.SemaphoreType.DMA((n,)),
            pltpu.SemaphoreType.DMA((2,)),
        ],
        compiler_params=pltpu.CompilerParams(
            collective_id=0, has_side_effects=True, vmem_limit_bytes=48 * 1024 * 1024),
    )(image, meta, table)
    return out


def extended(cells, sides, width):
    for axis, dim in sides:
        count = lax.axis_size(axis)
        head = lax.slice_in_dim(cells, 0, width, axis=dim)
        tail = lax.slice_in_dim(cells, cells.shape[dim] - width, cells.shape[dim], axis=dim)
        cells = jnp.concatenate(
            [
                lax.ppermute(tail, axis, [(i, (i + 1) % count) for i in range(count)]),
                cells,
                lax.ppermute(head, axis, [((i + 1) % count, i) for i in range(count)]),
            ],
            axis=dim,
        )
    return cells


def cubic_weights(shares):
    return (
        -shares * (shares - 1.0) * (shares - 2.0) / 6.0,
        (shares + 1.0) * (shares - 1.0) * (shares - 2.0) / 2.0,
        -(shares + 1.0) * shares * (shares - 2.0) / 2.0,
        (shares + 1.0) * shares * (shares - 1.0) / 6.0,
    )


def column_steps(image, offsets, frac_index, fractions):
    step_count = offsets.shape[0]
    all_shifts, all_index = (
        lax.all_gather(offsets, "gz", axis=1, tiled=True),
        lax.all_gather(frac_index, "gz", axis=1, tiled=True),
    )
    standing = jnp.swapaxes(
        lax.all_to_all(image, "gz", split_axis=2, concat_axis=0, tiled=True), 1, 2
    )
    total_planes = standing.shape[0]
    width_y = standing.shape[1]
    width_x = standing.shape[2]
    column_block = lax.axis_index("gz") * width_y // width_x
    block_pick = (jnp.arange(all_shifts.shape[3], dtype=jnp.int32) == column_block).astype(
        jnp.int32
    )
    levels = jnp.arange(total_planes, dtype=jnp.int32)
    table_rows = jnp.arange(fractions.shape[0], dtype=jnp.int32)
    for step_index in range(step_count):
        shifts_now = jnp.sum(all_shifts[step_index, :, 0, :] * block_pick[None, :], axis=1)
        index_now = jnp.sum(all_index[step_index, :, 0, :] * block_pick[None, :], axis=1)
        onehot = (index_now[:, None] == table_rows[None, :]).astype(jnp.float32)
        picked = jnp.dot(onehot, fractions, precision=lax.Precision.HIGHEST)
        zweights = cubic_weights(1.0 - picked[:, 0])
        xweights = cubic_weights(1.0 - picked[:, 1])
        yweights = cubic_weights(1.0 - picked[:, 2])
        rimmed = extended(standing, (("gz", 1), ("xy", 2)), 2)
        merged = jnp.zeros(rimmed.shape, jnp.float32)
        for node in range(4):
            source = jnp.mod(levels - shifts_now - 2 + node, total_planes)
            merged = merged + zweights[node][:, None, None] * jnp.take(rimmed, source, axis=0)
        along_y = jnp.zeros((total_planes, width_y, width_x + 4), jnp.float32)
        for node in range(4):
            along_y = along_y + yweights[node][:, None, None] * merged[:, node : node + width_y, :]
        along_x = jnp.zeros((total_planes, width_y, width_x), jnp.float32)
        for node in range(4):
            along_x = along_x + xweights[node][:, None, None] * along_y[:, :, node : node + width_x]
        standing = along_x
    return lax.all_to_all(
        jnp.swapaxes(standing, 1, 2), "gz", split_axis=0, concat_axis=2, tiled=True
    )


def solution(mesh):
    n, n_xy = mesh.shape["gz"], mesh.shape["xy"]

    def local(image, offsets, frac_index, fractions):
        planes, width, depth = image.shape
        block = depth // offsets.shape[3]
        if block == width == LANES and offsets.shape[2] == 1 and width % (8 * n) == 0 and n % 2 == 0 and n_xy % 2 == 0 and 2 * offsets.shape[0] <= HALO:
            return fused(image, offsets, frac_index, fractions, n, n_xy)
        return column_steps(image, offsets, frac_index, fractions)

    in_specs = (P("gz", "xy", None), P(None, "gz", "xy", None), P(None, "gz", "xy", None), P())
    out_specs = P("gz", "xy", None)
    return jax.shard_map(local, mesh=mesh, in_specs=in_specs, out_specs=out_specs, check_vma=False)
```
